32 devices in a mesh: blk: 8 (over y, x, core), tp: 4 (over z).
Axes of the slice: x: 2, y: 2, z: 4, core: 2. Of those that a mesh axis runs over, the one named last changes fastest.
Arguments:
- mantissa: bfloat16 [8, 2880, 2880], P('blk', 'tp'), may hold values from -6 to 6
- exponent: int32 [8, 2880, 90], P('blk', 'tp'), may hold values from -3 to 1
- home: int32 [8], replicated, may hold values from 0 to 7, as said below
- queries: bfloat16 [32, 4096], P('blk', 'tp'), may hold values from -8 to 8
- keys: bfloat16 [32, 2048, 512], P('blk', None, 'tp'), may hold values from -8 to 8
- values: bfloat16 [32, 2048, 512], P('blk', None, 'tp'), may hold values from -6 to 6
- lengths: int32 [32], P('blk'), may hold values from 2 to 2048
Outputs:
- served: bfloat16 [8, 2880, 2880], P('blk', 'tp')
- checks: float32 [8, 2880, 90], P('blk', 'tp')
- energy: float32 [8], P('blk')
- attended: bfloat16 [32, 4096], P('blk', 'tp')
The draws below stay inside these ranges and needn't reach their ends.
Inputs may be any that keep to these rules, and one draw needn't show every extreme that they name: home[e] = (e + r) mod 8 for one whole number r of 1 to 3, the same for every expert.
All inputs are finite; a program needn't handle non-finite values.
Results may differ from the reference program's by a relative error of at most 0.0095.
Values may be sent and summed in bfloat16 or wider, within the bound.
No kernel may reach another device: no remote copies, remote signals or barrier semaphores. Data moves between devices by JAX's collectives and lax.ppermute only.
A program may use at most 64 MiB of HBM per device.

```python
import jax
import jax.numpy as jnp
from jax import lax

D = 2880
F = 2880
QUERY_HEADS = 64
KEY_VALUE_HEADS = 8
HEAD_SIZE = 64
BLOCK = 32
GROUP = 4
CACHE_LENGTH = 2048
DB = 90
G = 8
DECODE_SEQUENCES = 32


def draw_keys(key, part):
    cache_table = jnp.clip(jax.random.normal(jax.random.fold_in(key, 11), (DECODE_SEQUENCES, CACHE_LENGTH, KEY_VALUE_HEADS * HEAD_SIZE), jnp.float32), -6.0, 6.0)
    return cache_table.astype(jnp.bfloat16)


def draw_queries(key, part):
    query_input = jnp.clip(jax.random.normal(jax.random.fold_in(key, 21), (DECODE_SEQUENCES, QUERY_HEADS * HEAD_SIZE), jnp.float32), -6.0, 6.0)
    return query_input.astype(jnp.bfloat16)


def draw_home(key, part):
    distance = jax.random.randint(jax.random.fold_in(key, 3), (), 1, GROUP)
    return ((jnp.arange(G) + distance) % G).astype(jnp.int32)


def draw_exponent(key, part):
    noise = jax.random.randint(jax.random.fold_in(key, 5), (G, F, DB), -3, 1)
    rising = 2 * jnp.arange(F) // F
    return (noise + rising[None, :, None]).astype(jnp.int32)


def plant(drawn, own_key, low, largest):
    longest = drawn.shape.index(max(drawn.shape))
    spots = []
    for shift in (0, 1):
        where = [jax.random.randint(jax.random.fold_in(own_key, axis), (), 0, length) for axis, length in enumerate(drawn.shape)]
        where[longest] = (where[longest] + shift) % drawn.shape[longest]
        spots.append(tuple(where))
    return drawn.at[spots[0]].set(low).at[spots[1]].set(largest)


def shard_levels(own_key, dims, cuts, least, largest):
    factor_of = 1.0
    for axis_at, blocks in cuts:
        steps = jax.random.uniform(jax.random.fold_in(jax.random.fold_in(own_key, 6), axis_at), (blocks,), jnp.float32, least / len(cuts), largest / len(cuts))
        factor_of = factor_of * jnp.repeat(jnp.exp(steps), dims[axis_at] // blocks).reshape((-1,) + (1,) * (len(dims) - 1 - axis_at))
    return factor_of


def gaussian(own_key, dims, scale, reach, split=(), held_as=jnp.bfloat16):
    drawn = scale * jax.random.normal(own_key, dims, jnp.float32)
    if split:
        drawn = drawn * shard_levels(own_key, dims, split, -0.22, 0.18)
    return jnp.clip(drawn, -reach, reach).astype(held_as)


def setup_inputs(seed: int = 0) -> dict:
    splits = jax.random.split(jax.random.key(seed), 8)
    return {
        "mantissa": gaussian(splits[0], (G, F, D), 1.0, 6.0, ((0, 8), (1, 4))),
        "exponent": draw_exponent(jax.random.fold_in(splits[7], 71), 0),
        "home": draw_home(jax.random.fold_in(splits[7], 71), 0),
        "queries": draw_queries(jax.random.fold_in(splits[7], 71), 0),
        "keys": draw_keys(jax.random.fold_in(splits[7], 71), 0),
        "values": gaussian(splits[5], (DECODE_SEQUENCES, CACHE_LENGTH, KEY_VALUE_HEADS * HEAD_SIZE), 1.0, 6.0, ((0, 8), (2, 4))),
        "lengths": plant(jax.random.randint(splits[6], (DECODE_SEQUENCES,), 2, CACHE_LENGTH + 1), jax.random.fold_in(splits[6], 1), 2, CACHE_LENGTH).astype(jnp.int32),
    }


def dequantize(mant, expo):
    scale = jnp.exp2(expo.astype(jnp.float32))
    blocks = mant.astype(jnp.float32).reshape(F, DB, BLOCK) * scale[:, :, None]
    return blocks.reshape(F, D).astype(jnp.bfloat16)


def reference(mantissa, exponent, home, queries, keys, values, lengths):
    slots = jnp.arange(G, dtype=jnp.int32)
    source = jnp.sum(jnp.where(home[None, :] == slots[:, None], slots[None, :], 0), axis=1).astype(jnp.int32)

    def serve_one(index):
        weights = dequantize(mantissa[index], exponent[index])
        wide = weights.astype(jnp.float32)
        sums = jnp.sum(wide.reshape(F, DB, BLOCK), axis=2)
        power = jnp.sum(wide * wide) / (F * D)
        return weights, sums, power

    served, checks, energy = lax.map(serve_one, source)

    query_groups = QUERY_HEADS // KEY_VALUE_HEADS
    query_input = queries.astype(jnp.float32).reshape(DECODE_SEQUENCES, KEY_VALUE_HEADS, query_groups, HEAD_SIZE)
    key_rows_full = keys.astype(jnp.float32).reshape(DECODE_SEQUENCES, CACHE_LENGTH, KEY_VALUE_HEADS, HEAD_SIZE)
    value_rows_full = values.astype(jnp.float32).reshape(DECODE_SEQUENCES, CACHE_LENGTH, KEY_VALUE_HEADS, HEAD_SIZE)
    scores = jnp.einsum("bgrh,blgh->bgrl", query_input, key_rows_full) * (HEAD_SIZE ** -0.5)
    live = jnp.arange(CACHE_LENGTH, dtype=jnp.int32)[None, :] < lengths[:, None]
    scores = jnp.where(live[:, None, None, :], scores, jnp.float32(-1e30))
    top = jnp.max(scores, axis=3, keepdims=True)
    expd = jnp.exp(scores - top)
    total = jnp.sum(expd, axis=3, keepdims=True)
    probs = (expd / total).astype(jnp.bfloat16)
    mixed = jnp.einsum("bgrl,blgh->bgrh", probs.astype(jnp.float32), value_rows_full)
    attended = mixed.astype(jnp.bfloat16).reshape(DECODE_SEQUENCES, QUERY_HEADS * HEAD_SIZE)
    return served, checks, energy, attended
```

```python
import functools

import jax
import jax.numpy as jnp
from jax import lax
from jax.experimental import pallas as pl
from jax.experimental.pallas import tpu as pltpu
from jax.sharding import PartitionSpec as P


HEAD_SIZE = 64
LARGEST_DISTANCE = 3
LANES = 128
SUBLANES = 16
FIRST = 112
HBM = pl.BlockSpec(memory_space=pltpu.HBM)
VMEM = pl.BlockSpec(memory_space=pltpu.VMEM)
SMEM = pl.BlockSpec(memory_space=pltpu.SMEM)
PARAMS = pltpu.CompilerParams(vmem_limit_bytes=16 * 2**20)


def tiles(first, last):
    marks = [first] + [mark for mark in range(0, last, LANES) if mark > first] + [last]
    return list(zip(marks[:-1], marks[1:]))


def membership(blocks, width):
    block = width // blocks
    offset = lax.broadcasted_iota(jnp.int32, (blocks, width), 1) - block * lax.broadcasted_iota(
        jnp.int32, (blocks, width), 0
    )
    return jnp.where((offset >= 0) & (offset < block), 1.0, 0.0).astype(jnp.bfloat16)


def packing(rows, width):
    columns, left = divmod(width, LANES)
    beside = LANES // left if left and LANES % left == 0 else 1
    group = -(-rows // (beside * SUBLANES)) * SUBLANES if left else 0
    return columns, left, min(group, rows), columns * rows + group


def packed_rows(first, last, width):
    return sum(packing(b - a, width)[3] for a, b in tiles(first, last))


def pack(narrow, out_buf, at):
    rows, width = narrow.shape
    columns, left, group, _ = packing(rows, width)
    for column in range(columns):
        out_buf[pl.ds(at + column * rows, rows)] = narrow[:, column * LANES : (column + 1) * LANES]
    for g, row in enumerate(range(0, rows, group) if left else ()):
        height = min(group, rows - row)
        out_buf[pl.ds(at + columns * rows, height), g * left : (g + 1) * left] = narrow[
            row : row + height, columns * LANES :
        ]


def unpack(packed, at, buf, first, rows):
    columns, left, group, _ = packing(rows, buf.shape[1])
    for column in range(columns):
        buf[pl.ds(first, rows), column * LANES : (column + 1) * LANES] = packed[pl.ds(at + column * rows, rows)]
    for g, row in enumerate(range(0, rows, group) if left else ()):
        height = min(group, rows - row)
        buf[pl.ds(first + row, height), columns * LANES :] = packed[
            pl.ds(at + columns * rows, height), g * left : (g + 1) * left
        ]


def scales(expo_ref, a, b):
    return jnp.exp2(expo_ref[:, 0, a:b].astype(jnp.float32)).astype(jnp.bfloat16)


def spread(scale, member):
    return lax.dot_general(scale, member, (((0,), (0,)), ((), ())), preferred_element_type=jnp.float32)


def sum_blocks(member, served):
    return lax.dot_general(member, served, (((1,), (1,)), ((), ())), preferred_element_type=jnp.float32)


def dequantize_kernel(chunks, scaled, counted, mant_hbm, expo_ref, before_ref, *refs):
    fresh_hbms, refs = refs[: len(chunks)], refs[len(chunks) :]
    power_ref, mant_buf, out_buf, in_sem, out_sem, scale_sem = refs
    blocks, width = expo_ref.shape[0], mant_hbm.shape[1]
    spans = [(k, a, b) for k, chunk in enumerate(chunks) for a, b in tiles(*chunk)]
    spans += [(None, a, b) for chunk in counted for a, b in tiles(*chunk)]
    loads, stores = [], []
    into = 0
    for n, (_, a, b) in enumerate(spans):
        load = pltpu.make_async_copy(
            mant_hbm.at[pl.ds(a, b - a)], mant_buf.at[pl.ds(into, b - a)], in_sem.at[n]
        )
        load.start()
        loads.append(load)
        into += b - a
    member = membership(blocks, width)
    power = jnp.zeros((SUBLANES, width), jnp.float32)
    at, into = 0, 0
    start = dict.fromkeys(range(len(chunks)), 0)
    if scaled:
        size = -(-blocks // SUBLANES) * SUBLANES
        end = out_buf.shape[0] - size
        out_buf[pl.ds(end, blocks), : scaled[1] - scaled[0]] = scales(expo_ref, *scaled)
        store = pltpu.make_async_copy(
            out_buf.at[pl.ds(end, size)], fresh_hbms[0].at[pl.ds(fresh_hbms[0].shape[0] - size, size)], scale_sem
        )
        store.start()
        stores.append(store)
    for n, (k, a, b) in enumerate(spans):
        rows = b - a
        wide = spread(scales(expo_ref, a, b), member)
        loads[n].wait()
        wide = mant_buf[pl.ds(into, rows)].astype(jnp.float32) * wide
        into += rows
        if k is not None:
            size = packing(rows, width)[3]
            pack(wide.astype(jnp.bfloat16), out_buf, at)
            store = pltpu.make_async_copy(
                out_buf.at[pl.ds(at, size)], fresh_hbms[k].at[pl.ds(start[k], size)], out_sem.at[n]
            )
            store.start()
            stores.append(store)
            at += size
            start[k] += size
        for row in range(0, rows, SUBLANES):
            power = power + wide[row : row + SUBLANES] * wide[row : row + SUBLANES]
    power_ref[0] = before_ref[0] + jnp.sum(power)
    for store in stores:
        store.wait()


def dequantize(mant, expo, before, chunks, sizes, scaled=None, counted=()):
    width = mant.shape[1]
    every = list(chunks) + list(counted)
    count = sum(len(tiles(*chunk)) for chunk in every)
    *fresh, power = pl.pallas_call(
        functools.partial(dequantize_kernel, chunks, scaled, counted),
        out_shape=tuple(jax.ShapeDtypeStruct((size, LANES), jnp.bfloat16) for size in sizes)
        + (jax.ShapeDtypeStruct((1,), jnp.float32),),
        in_specs=[HBM, VMEM, SMEM],
        out_specs=(HBM,) * len(chunks) + (SMEM,),
        scratch_shapes=[
            pltpu.VMEM((sum(b - a for a, b in every), width), jnp.bfloat16),
            pltpu.VMEM((sum(sizes), LANES), jnp.bfloat16),
            pltpu.SemaphoreType.DMA((count,)),
            pltpu.SemaphoreType.DMA((count,)),
            pltpu.SemaphoreType.DMA,
        ],
        compiler_params=PARAMS,
    )(mant, expo, before)
    return fresh, power


def attach_kernel(at, divisor, count, me_ref, *refs):
    power_refs, (_, out_hbm, buf, sem) = refs[:count], refs[count:]
    total = jnp.float32(0)
    for device in range(count):
        behind = lax.rem(me_ref[0] - device + count, count)
        one = power_refs[0][0]
        for n in range(1, count):
            one = jnp.where(behind == n, power_refs[n][0], one)
        total = total + one
    rest = jnp.full(buf.shape, total, jnp.float32) / divisor
    row = lax.broadcasted_iota(jnp.int32, buf.shape, 0)
    pieces = jnp.zeros(buf.shape, jnp.float32)
    for n in range(3):
        piece = rest.astype(jnp.bfloat16).astype(jnp.float32)
        rest = rest - piece
        pieces = jnp.where(row == n, piece, pieces)
    buf[...] = pieces.astype(jnp.bfloat16)
    copy = pltpu.make_async_copy(buf, out_hbm.at[pl.ds(at, buf.shape[0])], sem)
    copy.start()
    copy.wait()


def attach(me, powers, divisor, chunk):
    return pl.pallas_call(
        functools.partial(attach_kernel, chunk.shape[0] - SUBLANES, divisor, len(powers)),
        out_shape=jax.ShapeDtypeStruct(chunk.shape, chunk.dtype),
        in_specs=[SMEM] * (1 + len(powers)) + [HBM],
        out_specs=HBM,
        input_output_aliases={1 + len(powers): 0},
        scratch_shapes=[pltpu.VMEM((SUBLANES, LANES), jnp.bfloat16), pltpu.SemaphoreType.DMA],
        compiler_params=PARAMS,
        name="attach",
    )(me, *powers, chunk)


def receive_kernel(chunks, blocks, sources, has_outs, is_final, *refs):
    refs = list(refs)
    arrived = [[refs.pop(0) for _ in range(count)] for count in sources]
    if max(sources) > 1:
        which_ref = refs.pop(0)
    if has_outs:
        del refs[:2]
    if is_final:
        del refs[:1]
    served_hbm, checks_hbm = refs.pop(0), refs.pop(0)
    if is_final:
        energy_ref = refs.pop(0)
        del refs[:1]
    *packed, buf, sums_buf, in_sem, out_sem, sums_sem = refs
    width = buf.shape[1]
    first, last = chunks[0][0], chunks[-1][1]
    loads = []
    if is_final:
        packed = arrived[0]
    else:
        for n, one in enumerate(arrived):
            copies = [pltpu.make_async_copy(source, packed[n], in_sem.at[n]) for source in one]
            if len(copies) > 1:
                for k, copy in enumerate(copies):
                    pl.when(which_ref[0] == k)(copy.start)
            else:
                copies[0].start()
            loads.append(copies[0])
    member = membership(blocks, width)
    for load in loads:
        load.wait()
    stores = []
    if is_final:
        pieces = packed[0][pl.ds(packed[0].shape[0] - SUBLANES, SUBLANES), :].astype(jnp.float32)
        row = lax.broadcasted_iota(jnp.int32, pieces.shape, 0)
        pieces = jnp.sum(jnp.where(row < 3, pieces, 0.0), axis=0, keepdims=True)
        energy_ref[0] = pieces[0, 0]
    for n, chunk in enumerate(chunks):
        at = 0
        for a, b in tiles(*chunk):
            rows = b - a
            here = pl.ds(a - first, rows)
            if chunk[0] == 0:
                size = -(-blocks // SUBLANES) * SUBLANES
                scale = packed[1][pl.ds(packed[1].shape[0] - size, blocks), :rows]
                raw = packed[0][...].astype(jnp.float32)
                buf[here] = (raw * spread(scale, member)).astype(jnp.bfloat16)
            else:
                unpack(packed[n], at, buf, a - first, rows)
                at += packing(rows, width)[3]
            store = pltpu.make_async_copy(buf.at[here], served_hbm.at[pl.ds(a, rows)], out_sem.at[len(stores)])
            store.start()
            stores.append(store)
            sums_buf[:, 0, a - first : b - first] = sum_blocks(member, buf[here])
    store = pltpu.make_async_copy(sums_buf, checks_hbm.at[:, :, pl.ds(first, last - first)], sums_sem)
    store.start()
    stores.append(store)
    for store in stores:
        store.wait()


def receive(arrived, which, outs, attended, shape, blocks, chunks):
    rows, width = shape
    first, last = chunks[0][0], chunks[-1][1]
    count = sum(len(tiles(*chunk)) for chunk in chunks)
    is_final = attended is not None
    sources = [len(one) for one in arrived]
    operands = [(source, VMEM if is_final else HBM) for one in arrived for source in one]
    if max(sources) > 1:
        operands.append((which, SMEM))
    aliases = {len(operands) + n: n for n in range(len(outs))}
    operands += [(out, HBM) for out in outs]
    results = [
        (jax.ShapeDtypeStruct((rows, width), jnp.bfloat16), HBM),
        (jax.ShapeDtypeStruct((blocks, 1, rows), jnp.float32), HBM),
    ]
    if is_final:
        aliases[len(operands)] = 3
        operands.append((attended, HBM))
        results.append((jax.ShapeDtypeStruct((1,), jnp.float32), SMEM))
        results.append((jax.ShapeDtypeStruct(attended.shape, attended.dtype), HBM))
    return pl.pallas_call(
        functools.partial(receive_kernel, chunks, blocks, sources, bool(outs), is_final),
        out_shape=tuple(result for result, _ in results),
        in_specs=[spec for _, spec in operands],
        out_specs=tuple(spec for _, spec in results),
        input_output_aliases=aliases,
        scratch_shapes=([] if is_final else [pltpu.VMEM(one[0].shape, jnp.bfloat16) for one in arrived])
        + [
            pltpu.VMEM((last - first, width), jnp.bfloat16),
            pltpu.VMEM((blocks, 1, last - first), jnp.float32),
            pltpu.SemaphoreType.DMA((len(chunks),)),
            pltpu.SemaphoreType.DMA((count,)),
            pltpu.SemaphoreType.DMA,
        ],
        compiler_params=PARAMS,
    )(*[operand for operand, _ in operands])


def attend_kernel(lengths_ref, queries_ref, keys_hbm, values_hbm, out_hbm, keys_buf, values_buf, out_buf, sem, out_sem):
    seqs, slots_len, width = keys_hbm.shape
    span = queries_ref.shape[1]
    kv_heads = width // HEAD_SIZE
    heads = span // HEAD_SIZE
    each = span // kv_heads
    copies = []
    for seq in range(seqs):
        key_copy = pltpu.make_async_copy(keys_hbm.at[seq], keys_buf.at[seq], sem.at[0, seq])
        value_copy = pltpu.make_async_copy(values_hbm.at[seq], values_buf.at[seq], sem.at[1, seq])
        key_copy.start()
        value_copy.start()
        copies.append((key_copy, value_copy))
    at = lax.broadcasted_iota(jnp.int32, (heads, span), 1) - HEAD_SIZE * lax.broadcasted_iota(
        jnp.int32, (heads, span), 0
    )
    own = (at >= 0) & (at < HEAD_SIZE)
    column = lax.broadcasted_iota(jnp.int32, (span, width), 0)
    met = column % HEAD_SIZE
    for head in range(1, kv_heads):
        met = met + jnp.where(column >= head * each, HEAD_SIZE, 0)
    fold = jnp.where(met == lax.broadcasted_iota(jnp.int32, (span, width), 1), 1.0, 0.0).astype(jnp.bfloat16)
    slot = lax.broadcasted_iota(jnp.int32, (heads, slots_len), 1)
    for seq in range(seqs):
        query = jnp.where(own, queries_ref[seq : seq + 1, :].astype(jnp.float32), 0.0).astype(jnp.bfloat16)
        query = jnp.dot(query, fold, preferred_element_type=jnp.float32).astype(jnp.bfloat16)
        copies[seq][0].wait()
        scores = lax.dot_general(
            query, keys_buf[seq], (((1,), (1,)), ((), ())), preferred_element_type=jnp.float32
        ) * HEAD_SIZE ** (-0.5)
        scores = jnp.where(slot < lengths_ref[seq], scores, jnp.float32(-1e30))
        expd = jnp.exp(scores - jnp.max(scores, axis=1, keepdims=True))
        probs = (expd / jnp.sum(expd, axis=1, keepdims=True)).astype(jnp.bfloat16)
        copies[seq][1].wait()
        mixed = jnp.dot(probs, values_buf[seq], preferred_element_type=jnp.float32).astype(jnp.bfloat16)
        mixed = lax.dot_general(mixed, fold, (((1,), (1,)), ((), ())), preferred_element_type=jnp.float32)
        mixed = jnp.sum(jnp.where(own, mixed, 0.0), axis=0, keepdims=True)
        out_buf[seq : seq + 1, :] = mixed.astype(jnp.bfloat16)
    copy = pltpu.make_async_copy(out_buf, out_hbm, out_sem)
    copy.start()
    copy.wait()


def attend(queries, keys, values, lengths):
    return pl.pallas_call(
        attend_kernel,
        out_shape=jax.ShapeDtypeStruct(queries.shape, jnp.bfloat16),
        in_specs=[SMEM, VMEM, HBM, HBM],
        out_specs=HBM,
        scratch_shapes=[
            pltpu.VMEM(keys.shape, jnp.bfloat16),
            pltpu.VMEM(values.shape, jnp.bfloat16),
            pltpu.VMEM(queries.shape, jnp.bfloat16),
            pltpu.SemaphoreType.DMA((2, keys.shape[0])),
            pltpu.SemaphoreType.DMA,
        ],
        compiler_params=PARAMS,
        name="attend",
    )(lengths, queries, keys, values)


def shift(value, pairs, axis="blk"):
    return lax.ppermute(value, axis, pairs)


def plan(rows, relayed):
    if relayed:
        half = (rows // 2 + FIRST) // SUBLANES * SUBLANES
        marks = (0, FIRST, 2 * LANES, 3 * LANES, half, 5 * LANES, rows)
        groups = ((0, 1), (2,), (3, 4), (5,))
    else:
        marks = (0, FIRST, 3 * LANES, 5 * LANES, rows)
        groups = ((0, 1), (2,), (3,))
    return list(zip(marks[:-1], marks[1:])), (1, 2, 3) if relayed else (), groups


def refresh(distance, mant, expo, queries, keys, values, lengths):
    return refresh_from(distance, mant, expo, queries, keys, values, lengths)


def refresh_from(distance, mant, expo, queries, keys, values, lengths):
    count = lax.axis_size("blk")
    rows, width = mant.shape
    blocks = expo.shape[0]
    straight = [(i, (i + distance) % count) for i in range(count)]
    relayed = distance == 3 and count % 4 == 0
    bounds, by_relay, groups = plan(rows, relayed)
    to_relay = [(i, (i + 5) % count) for i in range(count) if i % 4 == 2]
    from_relay = [((i + 5) % count, (i + 3) % count) for i in range(count) if i % 4 == 2]
    others = [pair for pair in straight if pair[0] % 4 != 2]
    which = (lax.axis_index("blk") % 4 == 1).astype(jnp.int32).reshape(1)

    me = lax.axis_index("tp").reshape(1)

    sizes = [packed_rows(a, b, width) for a, b in bounds]
    sizes[1] += -(-blocks // SUBLANES) * SUBLANES
    sizes[-1] += SUBLANES
    power = jnp.zeros((1,), jnp.float32)
    fresh = [mant[: bounds[0][1]]]
    some, power = dequantize(mant, expo, power, bounds[1:2], sizes[1:2], scaled=bounds[0])
    fresh += some
    some, power = dequantize(mant, expo, power, bounds[2:], sizes[2:], counted=bounds[:1])
    fresh += some
    shards = lax.axis_size("tp")
    powers = [power] + [shift(power, [(i, (i + n) % shards) for i in range(shards)], "tp") for n in range(1, shards)]
    fresh[-1] = attach(me, powers, float(rows * shards * width), fresh[-1])
    arrived = []
    for n, chunk in enumerate(fresh):
        if n in by_relay:
            onward = shift(shift(chunk, to_relay), from_relay)
            arrived.append((shift(chunk, others), onward))
        else:
            arrived.append((shift(chunk, straight),))
    attended = attend(queries, keys, values, lengths)
    outs = []
    for group in groups:
        final = group[-1] == len(bounds) - 1
        outs = receive(
            [arrived[n] for n in group],
            which,
            outs,
            attended if final else None,
            (rows, width),
            blocks,
            [bounds[n] for n in group],
        )
    served, checks, energy, attended = outs
    return served, jnp.transpose(checks, (1, 2, 0)), energy, attended


def local(mantissa, exponent, home, queries, keys, values, lengths):
    rows, width = mantissa.shape[1:]
    mant = mantissa.reshape(rows, width)
    expo = jnp.transpose(exponent, (2, 0, 1))
    branches = [functools.partial(refresh, r) for r in range(1, LARGEST_DISTANCE + 1)]
    served, checks, energy, attended = lax.switch(
        home[0] - 1, branches, mant, expo, queries, keys, values, lengths
    )
    return served[None], checks, energy, attended


def solution(mesh):
    placed = (
        P("blk", "tp", None),
        P("blk", "tp", None),
        P(),
        P("blk", "tp"),
        P("blk", None, "tp"),
        P("blk", None, "tp"),
        P("blk"),
    )
    return jax.shard_map(
        local,
        mesh=mesh,
        in_specs=placed,
        out_specs=(P("blk", "tp", None), P("blk", "tp", None), P("blk"), P("blk", "tp")),
        check_vma=False,
    )
```

```python
import functools

import jax
import jax.numpy as jnp
from jax import lax
from jax.experimental import pallas as pl
from jax.experimental.pallas import tpu as pltpu
from jax.sharding import PartitionSpec as P


HEAD_SIZE = 64
LARGEST_DISTANCE = 3
LANES = 128
SUBLANES = 16
FIRST = {1: 112, 2: 64, 3: 112}
HBM = pl.BlockSpec(memory_space=pltpu.HBM)
VMEM = pl.BlockSpec(memory_space=pltpu.VMEM)
SMEM = pl.BlockSpec(memory_space=pltpu.SMEM)
PARAMS = pltpu.CompilerParams(vmem_limit_bytes=16 * 2**20)


def tiles(first, last):
    marks = [first] + [mark for mark in range(0, last, LANES) if mark > first] + [last]
    return list(zip(marks[:-1], marks[1:]))


def membership(blocks, width):
    block = width // blocks
    offset = lax.broadcasted_iota(jnp.int32, (blocks, width), 1) - block * lax.broadcasted_iota(
        jnp.int32, (blocks, width), 0
    )
    return jnp.where((offset >= 0) & (offset < block), 1.0, 0.0).astype(jnp.bfloat16)


def packing(rows, width):
    columns, left = divmod(width, LANES)
    beside = LANES // left if left and LANES % left == 0 else 1
    group = -(-rows // (beside * SUBLANES)) * SUBLANES if left else 0
    return columns, left, min(group, rows), columns * rows + group


def packed_rows(first, last, width):
    return sum(packing(b - a, width)[3] for a, b in tiles(first, last))


def pack(narrow, out_buf, at):
    rows, width = narrow.shape
    columns, left, group, _ = packing(rows, width)
    for column in range(columns):
        out_buf[pl.ds(at + column * rows, rows)] = narrow[:, column * LANES : (column + 1) * LANES]
    for g, row in enumerate(range(0, rows, group) if left else ()):
        height = min(group, rows - row)
        out_buf[pl.ds(at + columns * rows, height), g * left : (g + 1) * left] = narrow[
            row : row + height, columns * LANES :
        ]


def unpack(packed, at, buf, first, rows):
    columns, left, group, _ = packing(rows, buf.shape[1])
    for column in range(columns):
        buf[pl.ds(first, rows), column * LANES : (column + 1) * LANES] = packed[pl.ds(at + column * rows, rows)]
    for g, row in enumerate(range(0, rows, group) if left else ()):
        height = min(group, rows - row)
        buf[pl.ds(first + row, height), columns * LANES :] = packed[
            pl.ds(at + columns * rows, height), g * left : (g + 1) * left
        ]


def scales(expo_ref, a, b):
    return jnp.exp2(expo_ref[:, 0, a:b].astype(jnp.float32)).astype(jnp.bfloat16)


def spread(scale, member):
    return lax.dot_general(scale, member, (((0,), (0,)), ((), ())), preferred_element_type=jnp.float32)


def sum_blocks(member, served):
    return lax.dot_general(member, served, (((1,), (1,)), ((), ())), preferred_element_type=jnp.float32)


def take_kernel(spans, source_hbm, out_hbm, raw, packed, in_sem, out_sem):
    width = source_hbm.shape[1]
    loads, stores = [], []
    for n, (a, b) in enumerate(spans):
        load = pltpu.make_async_copy(source_hbm.at[pl.ds(a, b - a)], raw.at[pl.ds(a, b - a)], in_sem.at[n])
        load.start()
        loads.append(load)
    at = 0
    for n, (a, b) in enumerate(spans):
        size = packing(b - a, width)[3]
        loads[n].wait()
        pack(raw[pl.ds(a, b - a)], packed, at)
        store = pltpu.make_async_copy(packed.at[pl.ds(at, size)], out_hbm.at[pl.ds(at, size)], out_sem.at[n])
        store.start()
        stores.append(store)
        at += size
    for store in stores:
        store.wait()


def take(source, last, size):
    spans = tiles(0, last)
    return pl.pallas_call(
        functools.partial(take_kernel, spans),
        out_shape=jax.ShapeDtypeStruct((size, LANES), source.dtype),
        in_specs=[HBM],
        out_specs=HBM,
        scratch_shapes=[
            pltpu.VMEM((last, source.shape[1]), source.dtype),
            pltpu.VMEM((size, LANES), source.dtype),
            pltpu.SemaphoreType.DMA((len(spans),)),
            pltpu.SemaphoreType.DMA((len(spans),)),
        ],
        compiler_params=PARAMS,
        name="take",
    )(source)


def dequantize_kernel(chunks, scaled, counted, mant_hbm, expo_ref, before_ref, *refs):
    fresh_hbms, refs = refs[: len(chunks)], refs[len(chunks) :]
    power_ref, mant_buf, out_buf, in_sem, out_sem, scale_sem = refs
    blocks, width = expo_ref.shape[0], mant_hbm.shape[1]
    spans = [(k, a, b) for k, chunk in enumerate(chunks) for a, b in tiles(*chunk)]
    spans += [(None, a, b) for chunk in counted for a, b in tiles(*chunk)]
    loads, stores = [], []
    into = 0
    for n, (_, a, b) in enumerate(spans):
        load = pltpu.make_async_copy(
            mant_hbm.at[pl.ds(a, b - a)], mant_buf.at[pl.ds(into, b - a)], in_sem.at[n]
        )
        load.start()
        loads.append(load)
        into += b - a
    member = membership(blocks, width)
    power = jnp.zeros((SUBLANES, width), jnp.float32)
    at, into = 0, 0
    start = dict.fromkeys(range(len(chunks)), 0)
    if scaled:
        size = -(-blocks // SUBLANES) * SUBLANES
        end = out_buf.shape[0] - size
        out_buf[pl.ds(end, blocks), : scaled[1] - scaled[0]] = scales(expo_ref, *scaled)
        store = pltpu.make_async_copy(
            out_buf.at[pl.ds(end, size)], fresh_hbms[0].at[pl.ds(fresh_hbms[0].shape[0] - size, size)], scale_sem
        )
        store.start()
        stores.append(store)
    for n, (k, a, b) in enumerate(spans):
        rows = b - a
        wide = spread(scales(expo_ref, a, b), member)
        loads[n].wait()
        wide = mant_buf[pl.ds(into, rows)].astype(jnp.float32) * wide
        into += rows
        if k is not None:
            size = packing(rows, width)[3]
            pack(wide.astype(jnp.bfloat16), out_buf, at)
            store = pltpu.make_async_copy(
                out_buf.at[pl.ds(at, size)], fresh_hbms[k].at[pl.ds(start[k], size)], out_sem.at[n]
            )
            store.start()
            stores.append(store)
            at += size
            start[k] += size
        for row in range(0, rows, SUBLANES):
            power = power + wide[row : row + SUBLANES] * wide[row : row + SUBLANES]
    power_ref[0] = before_ref[0] + jnp.sum(power)
    for store in stores:
        store.wait()


def dequantize(mant, expo, before, chunks, sizes, scaled=None, counted=()):
    width = mant.shape[1]
    every = list(chunks) + list(counted)
    count = sum(len(tiles(*chunk)) for chunk in every)
    *fresh, power = pl.pallas_call(
        functools.partial(dequantize_kernel, chunks, scaled, counted),
        out_shape=tuple(jax.ShapeDtypeStruct((size, LANES), jnp.bfloat16) for size in sizes)
        + (jax.ShapeDtypeStruct((1,), jnp.float32),),
        in_specs=[HBM, VMEM, SMEM],
        out_specs=(HBM,) * len(chunks) + (SMEM,),
        scratch_shapes=[
            pltpu.VMEM((sum(b - a for a, b in every), width), jnp.bfloat16),
            pltpu.VMEM((sum(sizes), LANES), jnp.bfloat16),
            pltpu.SemaphoreType.DMA((count,)),
            pltpu.SemaphoreType.DMA((count,)),
            pltpu.SemaphoreType.DMA,
        ],
        compiler_params=PARAMS,
        name="dequantize_second" if scaled else "dequantize_rest",
    )(mant, expo, before)
    return fresh, power


def attach_kernel(at, divisor, count, me_ref, *refs):
    power_refs, (_, out_hbm, buf, sem) = refs[:count], refs[count:]
    total = jnp.float32(0)
    for device in range(count):
        behind = lax.rem(me_ref[0] - device + count, count)
        one = power_refs[0][0]
        for n in range(1, count):
            one = jnp.where(behind == n, power_refs[n][0], one)
        total = total + one
    rest = jnp.full(buf.shape, total, jnp.float32) / divisor
    row = lax.broadcasted_iota(jnp.int32, buf.shape, 0)
    pieces = jnp.zeros(buf.shape, jnp.float32)
    for n in range(3):
        piece = rest.astype(jnp.bfloat16).astype(jnp.float32)
        rest = rest - piece
        pieces = jnp.where(row == n, piece, pieces)
    buf[...] = pieces.astype(jnp.bfloat16)
    copy = pltpu.make_async_copy(buf, out_hbm.at[pl.ds(at, buf.shape[0])], sem)
    copy.start()
    copy.wait()


def attach(me, powers, divisor, chunk):
    return pl.pallas_call(
        functools.partial(attach_kernel, chunk.shape[0] - SUBLANES, divisor, len(powers)),
        out_shape=jax.ShapeDtypeStruct(chunk.shape, chunk.dtype),
        in_specs=[SMEM] * (1 + len(powers)) + [HBM],
        out_specs=HBM,
        input_output_aliases={1 + len(powers): 0},
        scratch_shapes=[pltpu.VMEM((SUBLANES, LANES), jnp.bfloat16), pltpu.SemaphoreType.DMA],
        compiler_params=PARAMS,
        name="attach",
    )(me, *powers, chunk)


def receive_kernel(chunks, blocks, sources, has_outs, is_final, direct, *refs):
    refs = list(refs)
    arrived = [[refs.pop(0) for _ in range(count)] for count in sources]
    if max(sources) > 1:
        which_ref = refs.pop(0)
    if has_outs:
        del refs[:2]
    if is_final:
        del refs[:1]
    served_hbm, checks_hbm = refs.pop(0), refs.pop(0)
    if is_final:
        energy_ref = refs.pop(0)
        del refs[:1]
    *packed, buf, sums_buf, in_sem, out_sem, sums_sem = refs
    width = buf.shape[1]
    first, last = chunks[0][0], chunks[-1][1]
    loads = []
    if direct:
        packed = [one[0] for one in arrived]
    else:
        for n, one in enumerate(arrived):
            copies = [pltpu.make_async_copy(source, packed[n], in_sem.at[n]) for source in one]
            if len(copies) > 1:
                for k, copy in enumerate(copies):
                    pl.when(which_ref[0] == k)(copy.start)
            else:
                copies[0].start()
            loads.append(copies[0])
    member = membership(blocks, width)
    stores = []
    for n, chunk in enumerate(chunks):
        at = 0
        while loads and (len(loads) == len(chunks) - n or chunk[0] == 0):
            loads.pop(0).wait()
        for a, b in tiles(*chunk):
            rows = b - a
            here = pl.ds(a - first, rows)
            unpack(packed[n], at, buf, a - first, rows)
            at += packing(rows, width)[3]
            if chunk[0] == 0:
                size = -(-blocks // SUBLANES) * SUBLANES
                scale = packed[1][pl.ds(packed[1].shape[0] - size, blocks), a:b]
                buf[here] = (buf[here].astype(jnp.float32) * spread(scale, member)).astype(jnp.bfloat16)
            store = pltpu.make_async_copy(buf.at[here], served_hbm.at[pl.ds(a, rows)], out_sem.at[len(stores)])
            store.start()
            stores.append(store)
            sums_buf[:, 0, a - first : b - first] = sum_blocks(member, buf[here])
    store = pltpu.make_async_copy(sums_buf, checks_hbm.at[:, :, pl.ds(first, last - first)], sums_sem)
    store.start()
    stores.append(store)
    if is_final:
        pieces = packed[-1][pl.ds(packed[-1].shape[0] - SUBLANES, SUBLANES), :].astype(jnp.float32)
        row = lax.broadcasted_iota(jnp.int32, pieces.shape, 0)
        pieces = jnp.sum(jnp.where(row < 3, pieces, 0.0), axis=0, keepdims=True)
        energy_ref[0] = pieces[0, 0]
    for store in stores:
        store.wait()


def receive(arrived, which, outs, attended, shape, blocks, chunks):
    rows, width = shape
    first, last = chunks[0][0], chunks[-1][1]
    count = sum(len(tiles(*chunk)) for chunk in chunks)
    is_final = attended is not None
    sources = [len(one) for one in arrived]
    direct = is_final and max(sources) == 1
    operands = [(source, VMEM if direct else HBM) for one in arrived for source in one]
    if max(sources) > 1:
        operands.append((which, SMEM))
    aliases = {len(operands) + n: n for n in range(len(outs))}
    operands += [(out, HBM) for out in outs]
    results = [
        (jax.ShapeDtypeStruct((rows, width), jnp.bfloat16), HBM),
        (jax.ShapeDtypeStruct((blocks, 1, rows), jnp.float32), HBM),
    ]
    if is_final:
        aliases[len(operands)] = 3
        operands.append((attended, HBM))
        results.append((jax.ShapeDtypeStruct((1,), jnp.float32), SMEM))
        results.append((jax.ShapeDtypeStruct(attended.shape, attended.dtype), HBM))
    return pl.pallas_call(
        functools.partial(receive_kernel, chunks, blocks, sources, bool(outs), is_final, direct),
        out_shape=tuple(result for result, _ in results),
        in_specs=[spec for _, spec in operands],
        out_specs=tuple(spec for _, spec in results),
        input_output_aliases=aliases,
        scratch_shapes=([] if direct else [pltpu.VMEM(one[0].shape, jnp.bfloat16) for one in arrived])
        + [
            pltpu.VMEM((last - first, width), jnp.bfloat16),
            pltpu.VMEM((blocks, 1, last - first), jnp.float32),
            pltpu.SemaphoreType.DMA((len(chunks),)),
            pltpu.SemaphoreType.DMA((count,)),
            pltpu.SemaphoreType.DMA,
        ],
        compiler_params=PARAMS,
    )(*[operand for operand, _ in operands])


def attend_kernel(lengths_ref, queries_ref, keys_hbm, values_hbm, out_hbm, keys_buf, values_buf, out_buf, sem, out_sem):
    seqs, slots_len, width = keys_hbm.shape
    span = queries_ref.shape[1]
    kv_heads = width // HEAD_SIZE
    heads = span // HEAD_SIZE
    each = span // kv_heads
    copies = []
    for seq in range(seqs):
        key_copy = pltpu.make_async_copy(keys_hbm.at[seq], keys_buf.at[seq], sem.at[0, seq])
        value_copy = pltpu.make_async_copy(values_hbm.at[seq], values_buf.at[seq], sem.at[1, seq])
        key_copy.start()
        value_copy.start()
        copies.append((key_copy, value_copy))
    at = lax.broadcasted_iota(jnp.int32, (heads, span), 1) - HEAD_SIZE * lax.broadcasted_iota(
        jnp.int32, (heads, span), 0
    )
    own = (at >= 0) & (at < HEAD_SIZE)
    column = lax.broadcasted_iota(jnp.int32, (span, width), 0)
    met = column % HEAD_SIZE
    for head in range(1, kv_heads):
        met = met + jnp.where(column >= head * each, HEAD_SIZE, 0)
    fold = jnp.where(met == lax.broadcasted_iota(jnp.int32, (span, width), 1), 1.0, 0.0).astype(jnp.bfloat16)
    slot = lax.broadcasted_iota(jnp.int32, (heads, slots_len), 1)
    for seq in range(seqs):
        query = jnp.where(own, queries_ref[seq : seq + 1, :].astype(jnp.float32), 0.0).astype(jnp.bfloat16)
        query = jnp.dot(query, fold, preferred_element_type=jnp.float32).astype(jnp.bfloat16)
        copies[seq][0].wait()
        scores = lax.dot_general(
            query, keys_buf[seq], (((1,), (1,)), ((), ())), preferred_element_type=jnp.float32
        ) * HEAD_SIZE ** (-0.5)
        scores = jnp.where(slot < lengths_ref[seq], scores, jnp.float32(-1e30))
        expd = jnp.exp(scores - jnp.max(scores, axis=1, keepdims=True))
        probs = (expd / jnp.sum(expd, axis=1, keepdims=True)).astype(jnp.bfloat16)
        copies[seq][1].wait()
        mixed = jnp.dot(probs, values_buf[seq], preferred_element_type=jnp.float32).astype(jnp.bfloat16)
        mixed = lax.dot_general(mixed, fold, (((1,), (1,)), ((), ())), preferred_element_type=jnp.float32)
        mixed = jnp.sum(jnp.where(own, mixed, 0.0), axis=0, keepdims=True)
        out_buf[seq : seq + 1, :] = mixed.astype(jnp.bfloat16)
    copy = pltpu.make_async_copy(out_buf, out_hbm, out_sem)
    copy.start()
    copy.wait()


def attend(queries, keys, values, lengths):
    return pl.pallas_call(
        attend_kernel,
        out_shape=jax.ShapeDtypeStruct(queries.shape, jnp.bfloat16),
        in_specs=[SMEM, VMEM, HBM, HBM],
        out_specs=HBM,
        scratch_shapes=[
            pltpu.VMEM(keys.shape, jnp.bfloat16),
            pltpu.VMEM(values.shape, jnp.bfloat16),
            pltpu.VMEM(queries.shape, jnp.bfloat16),
            pltpu.SemaphoreType.DMA((2, keys.shape[0])),
            pltpu.SemaphoreType.DMA,
        ],
        compiler_params=PARAMS,
        name="attend",
    )(lengths, queries, keys, values)


def shift(value, pairs, axis="blk"):
    return lax.ppermute(value, axis, pairs)


def plan(rows, distance, relayed):
    first = FIRST[distance]
    if relayed:
        half = (rows // 2 + 2 * first) // SUBLANES * SUBLANES
        marks = (0, first, 2 * LANES, 3 * LANES, 4 * LANES, half, rows)
        groups = ((0, 1), (2,), (3,), (4, 5))
    else:
        marks = (0, first, 3 * LANES, 5 * LANES, rows)
        groups = ((0, 1), (2,), (3,))
    return list(zip(marks[:-1], marks[1:])), (1, 2, 4) if relayed else (), groups


def refresh(distance, mant, expo, queries, keys, values, lengths):
    return refresh_from(distance, mant, expo, queries, keys, values, lengths)


def refresh_from(distance, mant, expo, queries, keys, values, lengths):
    count = lax.axis_size("blk")
    rows, width = mant.shape
    blocks = expo.shape[0]
    straight = [(i, (i + distance) % count) for i in range(count)]
    relayed = distance == 3 and count % 4 == 0
    bounds, by_relay, groups = plan(rows, distance, relayed)
    to_relay = [(i, (i + 5) % count) for i in range(count) if i % 4 == 2]
    from_relay = [((i + 5) % count, (i + 3) % count) for i in range(count) if i % 4 == 2]
    others = [pair for pair in straight if pair[0] % 4 != 2]
    which = (lax.axis_index("blk") % 4 == 1).astype(jnp.int32).reshape(1)

    me = lax.axis_index("tp").reshape(1)

    sizes = [packed_rows(a, b, width) for a, b in bounds]
    sizes[1] += -(-blocks // SUBLANES) * SUBLANES
    sizes[-1] += SUBLANES
    power = jnp.zeros((1,), jnp.float32)
    fresh = [take(mant, bounds[0][1], sizes[0])]
    some, power = dequantize(mant, expo, power, bounds[1:2], sizes[1:2], scaled=bounds[0])
    fresh += some
    some, power = dequantize(mant, expo, power, bounds[2:], sizes[2:], counted=bounds[:1])
    fresh += some
    shards = lax.axis_size("tp")
    powers = [power] + [shift(power, [(i, (i + n) % shards) for i in range(shards)], "tp") for n in range(1, shards)]
    fresh[-1] = attach(me, powers, float(rows * shards * width), fresh[-1])
    arrived = []
    for n, chunk in enumerate(fresh):
        if n in by_relay:
            onward = shift(shift(chunk, to_relay), from_relay)
            arrived.append((shift(chunk, others), onward))
        else:
            arrived.append((shift(chunk, straight),))
    attended = attend(queries, keys, values, lengths)
    outs = []
    for group in groups:
        final = group[-1] == len(bounds) - 1
        outs = receive(
            [arrived[n] for n in group],
            which,
            outs,
            attended if final else None,
            (rows, width),
            blocks,
            [bounds[n] for n in group],
        )
    served, checks, energy, attended = outs
    return served, jnp.transpose(checks, (1, 2, 0)), energy, attended


def local(mantissa, exponent, home, queries, keys, values, lengths):
    rows, width = mantissa.shape[1:]
    mant = mantissa.reshape(rows, width)
    expo = jnp.transpose(exponent, (2, 0, 1))
    branches = [functools.partial(refresh, r) for r in range(1, LARGEST_DISTANCE + 1)]
    served, checks, energy, attended = lax.switch(
        home[0] - 1, branches, mant, expo, queries, keys, values, lengths
    )
    return served[None], checks, energy, attended


def solution(mesh):
    placed = (
        P("blk", "tp", None),
        P("blk", "tp", None),
        P(),
        P("blk", "tp"),
        P("blk", None, "tp"),
        P("blk", None, "tp"),
        P("blk"),
    )
    return jax.shard_map(
        local,
        mesh=mesh,
        in_specs=placed,
        out_specs=(P("blk", "tp", None), P("blk", "tp", None), P("blk"), P("blk", "tp")),
        check_vma=False,
    )
```

```python
import functools

import jax
import jax.numpy as jnp
from jax import lax
from jax.experimental import pallas as pl
from jax.experimental.pallas import tpu as pltpu
from jax.sharding import PartitionSpec as P


HEAD_SIZE = 64
LARGEST_DISTANCE = 3
LANES = 128
SUBLANES = 16
PIECE = 32
FIRST = {1: 112, 2: 64, 3: 112}
HBM = pl.BlockSpec(memory_space=pltpu.HBM)
VMEM = pl.BlockSpec(memory_space=pltpu.VMEM)
SMEM = pl.BlockSpec(memory_space=pltpu.SMEM)
PARAMS = pltpu.CompilerParams(vmem_limit_bytes=16 * 2**20)


def tiles(first, last):
    step = LANES if first or last > LANES else PIECE
    marks = [first] + [mark for mark in range(0, last, step) if mark > first] + [last]
    return list(zip(marks[:-1], marks[1:]))


def membership(blocks, width):
    block = width // blocks
    offset = lax.broadcasted_iota(jnp.int32, (blocks, width), 1) - block * lax.broadcasted_iota(
        jnp.int32, (blocks, width), 0
    )
    return jnp.where((offset >= 0) & (offset < block), 1.0, 0.0).astype(jnp.bfloat16)


def packing(rows, width):
    columns, left = divmod(width, LANES)
    beside = LANES // left if left and LANES % left == 0 else 1
    group = -(-rows // (beside * SUBLANES)) * SUBLANES if left else 0
    return columns, left, min(group, rows), columns * rows + group


def packed_rows(first, last, width):
    return sum(packing(b - a, width)[3] for a, b in tiles(first, last))


def pack(narrow, out_buf, at):
    rows, width = narrow.shape
    columns, left, group, _ = packing(rows, width)
    for column in range(columns):
        out_buf[pl.ds(at + column * rows, rows)] = narrow[:, column * LANES : (column + 1) * LANES]
    for g, row in enumerate(range(0, rows, group) if left else ()):
        height = min(group, rows - row)
        out_buf[pl.ds(at + columns * rows, height), g * left : (g + 1) * left] = narrow[
            row : row + height, columns * LANES :
        ]


def unpack(packed, at, buf, first, rows):
    columns, left, group, _ = packing(rows, buf.shape[1])
    for column in range(columns):
        buf[pl.ds(first, rows), column * LANES : (column + 1) * LANES] = packed[pl.ds(at + column * rows, rows)]
    for g, row in enumerate(range(0, rows, group) if left else ()):
        height = min(group, rows - row)
        buf[pl.ds(first + row, height), columns * LANES :] = packed[
            pl.ds(at + columns * rows, height), g * left : (g + 1) * left
        ]


def scales(expo_ref, a, b):
    return jnp.exp2(expo_ref[:, 0, a:b].astype(jnp.float32)).astype(jnp.bfloat16)


def spread(scale, member):
    return lax.dot_general(scale, member, (((0,), (0,)), ((), ())), preferred_element_type=jnp.float32)


def sum_blocks(member, served):
    return lax.dot_general(member, served, (((1,), (1,)), ((), ())), preferred_element_type=jnp.float32)


def take_kernel(spans, source_hbm, out_hbm, raw, packed, in_sem, out_sem):
    width = source_hbm.shape[1]
    loads, stores = [], []
    for n, (a, b) in enumerate(spans):
        load = pltpu.make_async_copy(source_hbm.at[pl.ds(a, b - a)], raw.at[pl.ds(a, b - a)], in_sem.at[n])
        load.start()
        loads.append(load)
    at = 0
    for n, (a, b) in enumerate(spans):
        size = packing(b - a, width)[3]
        loads[n].wait()
        pack(raw[pl.ds(a, b - a)], packed, at)
        store = pltpu.make_async_copy(packed.at[pl.ds(at, size)], out_hbm.at[pl.ds(at, size)], out_sem.at[n])
        store.start()
        stores.append(store)
        at += size
    for store in stores:
        store.wait()


def take(source, last, size):
    spans = tiles(0, last)
    return pl.pallas_call(
        functools.partial(take_kernel, spans),
        out_shape=jax.ShapeDtypeStruct((size, LANES), source.dtype),
        in_specs=[HBM],
        out_specs=HBM,
        scratch_shapes=[
            pltpu.VMEM((last, source.shape[1]), source.dtype),
            pltpu.VMEM((size, LANES), source.dtype),
            pltpu.SemaphoreType.DMA((len(spans),)),
            pltpu.SemaphoreType.DMA((len(spans),)),
        ],
        compiler_params=PARAMS,
        name="take",
    )(source)


def dequantize_kernel(chunks, scaled, counted, mant_hbm, expo_ref, before_ref, *refs):
    fresh_hbms, refs = refs[: len(chunks)], refs[len(chunks) :]
    power_ref, mant_buf, out_buf, in_sem, out_sem, scale_sem = refs
    blocks, width = expo_ref.shape[0], mant_hbm.shape[1]
    spans = [(k, a, b) for k, chunk in enumerate(chunks) for a, b in tiles(*chunk)]
    spans += [(None, a, b) for chunk in counted for a, b in tiles(*chunk)]
    loads, stores = [], []
    into = 0
    for n, (_, a, b) in enumerate(spans):
        load = pltpu.make_async_copy(
            mant_hbm.at[pl.ds(a, b - a)], mant_buf.at[pl.ds(into, b - a)], in_sem.at[n]
        )
        load.start()
        loads.append(load)
        into += b - a
    member = membership(blocks, width)
    power = jnp.zeros((SUBLANES, width), jnp.float32)
    at, into = 0, 0
    start = dict.fromkeys(range(len(chunks)), 0)
    if scaled:
        size = -(-blocks // SUBLANES) * SUBLANES
        end = out_buf.shape[0] - size
        out_buf[pl.ds(end, blocks), : scaled[1] - scaled[0]] = scales(expo_ref, *scaled)
        store = pltpu.make_async_copy(
            out_buf.at[pl.ds(end, size)], fresh_hbms[0].at[pl.ds(fresh_hbms[0].shape[0] - size, size)], scale_sem
        )
        store.start()
        stores.append(store)
    for n, (k, a, b) in enumerate(spans):
        rows = b - a
        wide = spread(scales(expo_ref, a, b), member)
        loads[n].wait()
        wide = mant_buf[pl.ds(into, rows)].astype(jnp.float32) * wide
        into += rows
        if k is not None:
            size = packing(rows, width)[3]
            pack(wide.astype(jnp.bfloat16), out_buf, at)
            store = pltpu.make_async_copy(
                out_buf.at[pl.ds(at, size)], fresh_hbms[k].at[pl.ds(start[k], size)], out_sem.at[n]
            )
            store.start()
            stores.append(store)
            at += size
            start[k] += size
        for row in range(0, rows, SUBLANES):
            power = power + wide[row : row + SUBLANES] * wide[row : row + SUBLANES]
    power_ref[0] = before_ref[0] + jnp.sum(power)
    for store in stores:
        store.wait()


def dequantize(mant, expo, before, chunks, sizes, scaled=None, counted=()):
    width = mant.shape[1]
    every = list(chunks) + list(counted)
    count = sum(len(tiles(*chunk)) for chunk in every)
    *fresh, power = pl.pallas_call(
        functools.partial(dequantize_kernel, chunks, scaled, counted),
        out_shape=tuple(jax.ShapeDtypeStruct((size, LANES), jnp.bfloat16) for size in sizes)
        + (jax.ShapeDtypeStruct((1,), jnp.float32),),
        in_specs=[HBM, VMEM, SMEM],
        out_specs=(HBM,) * len(chunks) + (SMEM,),
        scratch_shapes=[
            pltpu.VMEM((sum(b - a for a, b in every), width), jnp.bfloat16),
            pltpu.VMEM((sum(sizes), LANES), jnp.bfloat16),
            pltpu.SemaphoreType.DMA((count,)),
            pltpu.SemaphoreType.DMA((count,)),
            pltpu.SemaphoreType.DMA,
        ],
        compiler_params=PARAMS,
        name="dequantize_second" if scaled else "dequantize_rest",
    )(mant, expo, before)
    return fresh, power


def attach_kernel(at, divisor, count, me_ref, *refs):
    power_refs, (_, out_hbm, buf, sem) = refs[:count], refs[count:]
    total = jnp.float32(0)
    for device in range(count):
        behind = lax.rem(me_ref[0] - device + count, count)
        one = power_refs[0][0]
        for n in range(1, count):
            one = jnp.where(behind == n, power_refs[n][0], one)
        total = total + one
    rest = jnp.full(buf.shape, total, jnp.float32) / divisor
    row = lax.broadcasted_iota(jnp.int32, buf.shape, 0)
    pieces = jnp.zeros(buf.shape, jnp.float32)
    for n in range(3):
        piece = rest.astype(jnp.bfloat16).astype(jnp.float32)
        rest = rest - piece
        pieces = jnp.where(row == n, piece, pieces)
    buf[...] = pieces.astype(jnp.bfloat16)
    copy = pltpu.make_async_copy(buf, out_hbm.at[pl.ds(at, buf.shape[0])], sem)
    copy.start()
    copy.wait()


def attach(me, powers, divisor, chunk):
    return pl.pallas_call(
        functools.partial(attach_kernel, chunk.shape[0] - SUBLANES, divisor, len(powers)),
        out_shape=jax.ShapeDtypeStruct(chunk.shape, chunk.dtype),
        in_specs=[SMEM] * (1 + len(powers)) + [HBM],
        out_specs=HBM,
        input_output_aliases={1 + len(powers): 0},
        scratch_shapes=[pltpu.VMEM((SUBLANES, LANES), jnp.bfloat16), pltpu.SemaphoreType.DMA],
        compiler_params=PARAMS,
        name="attach",
    )(me, *powers, chunk)


def receive_kernel(chunks, blocks, sources, has_outs, is_final, direct, *refs):
    refs = list(refs)
    arrived = [[refs.pop(0) for _ in range(count)] for count in sources]
    if max(sources) > 1:
        which_ref = refs.pop(0)
    if has_outs:
        del refs[:2]
    if is_final:
        del refs[:1]
    served_hbm, checks_hbm = refs.pop(0), refs.pop(0)
    if is_final:
        energy_ref = refs.pop(0)
        del refs[:1]
    *packed, buf, sums_buf, in_sem, out_sem, sums_sem = refs
    chosen = list(packed)
    width = buf.shape[1]
    first, last = chunks[0][0], chunks[-1][1]
    loads = []
    for n, one in enumerate(() if direct else arrived):
        copies = [pltpu.make_async_copy(source, packed[n], in_sem.at[n]) for source in one]
        if len(copies) > 1:
            for k, copy in enumerate(copies):
                pl.when(which_ref[0] == k)(copy.start)
        else:
            copies[0].start()
        loads.append(copies[0])
    if direct:
        packed = []
        for one in arrived:
            if len(one) == 1:
                packed.append(one[0])
            else:
                packed.append(chosen.pop(0))
                for k, source in enumerate(one):

                    @pl.when(which_ref[0] == k)
                    def _(source=source, into=packed[-1]):
                        into[...] = source[...]

    member = membership(blocks, width)
    stores = []
    for n, chunk in enumerate(chunks):
        at = 0
        while loads and (len(loads) == len(chunks) - n or chunk[0] == 0):
            loads.pop(0).wait()
        for a, b in tiles(*chunk):
            rows = b - a
            here = pl.ds(a - first, rows)
            unpack(packed[n], at, buf, a - first, rows)
            at += packing(rows, width)[3]
            if chunk[0] == 0:
                size = -(-blocks // SUBLANES) * SUBLANES
                scale = packed[1][pl.ds(packed[1].shape[0] - size, blocks), a:b]
                buf[here] = (buf[here].astype(jnp.float32) * spread(scale, member)).astype(jnp.bfloat16)
            store = pltpu.make_async_copy(buf.at[here], served_hbm.at[pl.ds(a, rows)], out_sem.at[len(stores)])
            store.start()
            stores.append(store)
            sums_buf[:, 0, a - first : b - first] = sum_blocks(member, buf[here])
    store = pltpu.make_async_copy(sums_buf, checks_hbm.at[:, :, pl.ds(first, last - first)], sums_sem)
    store.start()
    stores.append(store)
    if is_final:
        pieces = packed[-1][pl.ds(packed[-1].shape[0] - SUBLANES, SUBLANES), :].astype(jnp.float32)
        row = lax.broadcasted_iota(jnp.int32, pieces.shape, 0)
        pieces = jnp.sum(jnp.where(row < 3, pieces, 0.0), axis=0, keepdims=True)
        energy_ref[0] = pieces[0, 0]
    for store in stores:
        store.wait()


def receive(arrived, which, outs, attended, shape, blocks, chunks):
    rows, width = shape
    first, last = chunks[0][0], chunks[-1][1]
    count = sum(len(tiles(*chunk)) for chunk in chunks)
    is_final = attended is not None
    sources = [len(one) for one in arrived]
    direct = is_final
    operands = [(source, VMEM if direct else HBM) for one in arrived for source in one]
    if max(sources) > 1:
        operands.append((which, SMEM))
    aliases = {len(operands) + n: n for n in range(len(outs))}
    operands += [(out, HBM) for out in outs]
    results = [
        (jax.ShapeDtypeStruct((rows, width), jnp.bfloat16), HBM),
        (jax.ShapeDtypeStruct((blocks, 1, rows), jnp.float32), HBM),
    ]
    if is_final:
        aliases[len(operands)] = 3
        operands.append((attended, HBM))
        results.append((jax.ShapeDtypeStruct((1,), jnp.float32), SMEM))
        results.append((jax.ShapeDtypeStruct(attended.shape, attended.dtype), HBM))
    return pl.pallas_call(
        functools.partial(receive_kernel, chunks, blocks, sources, bool(outs), is_final, direct),
        out_shape=tuple(result for result, _ in results),
        in_specs=[spec for _, spec in operands],
        out_specs=tuple(spec for _, spec in results),
        input_output_aliases=aliases,
        scratch_shapes=[pltpu.VMEM(one[0].shape, jnp.bfloat16) for one in arrived if len(one) > 1 or not direct]
        + [
            pltpu.VMEM((last - first, width), jnp.bfloat16),
            pltpu.VMEM((blocks, 1, last - first), jnp.float32),
            pltpu.SemaphoreType.DMA((len(chunks),)),
            pltpu.SemaphoreType.DMA((count,)),
            pltpu.SemaphoreType.DMA,
        ],
        compiler_params=PARAMS,
    )(*[operand for operand, _ in operands])


def attend_kernel(lengths_ref, queries_ref, keys_hbm, values_hbm, out_hbm, keys_buf, values_buf, out_buf, sem, out_sem):
    seqs, slots_len, width = keys_hbm.shape
    span = queries_ref.shape[1]
    kv_heads = width // HEAD_SIZE
    heads = span // HEAD_SIZE
    each = span // kv_heads
    copies = []
    for seq in range(seqs):
        key_copy = pltpu.make_async_copy(keys_hbm.at[seq], keys_buf.at[seq], sem.at[0, seq])
        value_copy = pltpu.make_async_copy(values_hbm.at[seq], values_buf.at[seq], sem.at[1, seq])
        key_copy.start()
        value_copy.start()
        copies.append((key_copy, value_copy))
    at = lax.broadcasted_iota(jnp.int32, (heads, span), 1) - HEAD_SIZE * lax.broadcasted_iota(
        jnp.int32, (heads, span), 0
    )
    own = (at >= 0) & (at < HEAD_SIZE)
    column = lax.broadcasted_iota(jnp.int32, (span, width), 0)
    met = column % HEAD_SIZE
    for head in range(1, kv_heads):
        met = met + jnp.where(column >= head * each, HEAD_SIZE, 0)
    fold = jnp.where(met == lax.broadcasted_iota(jnp.int32, (span, width), 1), 1.0, 0.0).astype(jnp.bfloat16)
    slot = lax.broadcasted_iota(jnp.int32, (heads, slots_len), 1)
    for seq in range(seqs):
        query = jnp.where(own, queries_ref[seq : seq + 1, :].astype(jnp.float32), 0.0).astype(jnp.bfloat16)
        query = jnp.dot(query, fold, preferred_element_type=jnp.float32).astype(jnp.bfloat16)
        copies[seq][0].wait()
        scores = lax.dot_general(
            query, keys_buf[seq], (((1,), (1,)), ((), ())), preferred_element_type=jnp.float32
        ) * HEAD_SIZE ** (-0.5)
        scores = jnp.where(slot < lengths_ref[seq], scores, jnp.float32(-1e30))
        expd = jnp.exp(scores - jnp.max(scores, axis=1, keepdims=True))
        probs = (expd / jnp.sum(expd, axis=1, keepdims=True)).astype(jnp.bfloat16)
        copies[seq][1].wait()
        mixed = jnp.dot(probs, values_buf[seq], preferred_element_type=jnp.float32).astype(jnp.bfloat16)
        mixed = lax.dot_general(mixed, fold, (((1,), (1,)), ((), ())), preferred_element_type=jnp.float32)
        mixed = jnp.sum(jnp.where(own, mixed, 0.0), axis=0, keepdims=True)
        out_buf[seq : seq + 1, :] = mixed.astype(jnp.bfloat16)
    copy = pltpu.make_async_copy(out_buf, out_hbm, out_sem)
    copy.start()
    copy.wait()


def attend(queries, keys, values, lengths):
    return pl.pallas_call(
        attend_kernel,
        out_shape=jax.ShapeDtypeStruct(queries.shape, jnp.bfloat16),
        in_specs=[SMEM, VMEM, HBM, HBM],
        out_specs=HBM,
        scratch_shapes=[
            pltpu.VMEM(keys.shape, jnp.bfloat16),
            pltpu.VMEM(values.shape, jnp.bfloat16),
            pltpu.VMEM(queries.shape, jnp.bfloat16),
            pltpu.SemaphoreType.DMA((2, keys.shape[0])),
            pltpu.SemaphoreType.DMA,
        ],
        compiler_params=PARAMS,
        name="attend",
    )(lengths, queries, keys, values)


def shift(value, pairs, axis="blk"):
    return lax.ppermute(value, axis, pairs)


def plan(rows, distance, relayed):
    first = FIRST[distance]
    if relayed:
        half = -(-rows // 2 // SUBLANES) * SUBLANES
        marks = (0, first, 2 * LANES, 3 * LANES, 8 * LANES - first - half, 5 * LANES, rows)
        groups = ((0, 1), (2,), (3, 4), (5,))
    else:
        marks = (0, first, 3 * LANES, 5 * LANES, rows)
        groups = ((0, 1), (2,), (3,))
    return list(zip(marks[:-1], marks[1:])), (1, 2, 4) if relayed else (), groups


def refresh(distance, mant, expo, queries, keys, values, lengths):
    return refresh_from(distance, mant, expo, queries, keys, values, lengths)


def refresh_from(distance, mant, expo, queries, keys, values, lengths):
    count = lax.axis_size("blk")
    rows, width = mant.shape
    blocks = expo.shape[0]
    straight = [(i, (i + distance) % count) for i in range(count)]
    relayed = distance == 3 and count % 4 == 0
    bounds, by_relay, groups = plan(rows, distance, relayed)
    to_relay = [(i, (i + 5) % count) for i in range(count) if i % 4 == 2]
    from_relay = [((i + 5) % count, (i + 3) % count) for i in range(count) if i % 4 == 2]
    others = [pair for pair in straight if pair[0] % 4 != 2]
    which = (lax.axis_index("blk") % 4 == 1).astype(jnp.int32).reshape(1)

    me = lax.axis_index("tp").reshape(1)

    sizes = [packed_rows(a, b, width) for a, b in bounds]
    sizes[1] += -(-blocks // SUBLANES) * SUBLANES
    sizes[-1] += SUBLANES
    power = jnp.zeros((1,), jnp.float32)
    fresh = [take(mant, bounds[0][1], sizes[0])]
    some, power = dequantize(mant, expo, power, bounds[1:2], sizes[1:2], scaled=bounds[0])
    fresh += some
    some, power = dequantize(mant, expo, power, bounds[2:], sizes[2:], counted=bounds[:1])
    fresh += some
    shards = lax.axis_size("tp")
    powers = [power] + [shift(power, [(i, (i + n) % shards) for i in range(shards)], "tp") for n in range(1, shards)]
    fresh[-1] = attach(me, powers, float(rows * shards * width), fresh[-1])
    arrived = []
    for n, chunk in enumerate(fresh):
        if n in by_relay:
            onward = shift(shift(chunk, to_relay), from_relay)
            arrived.append((shift(chunk, others), onward))
        else:
            arrived.append((shift(chunk, straight),))
    attended = attend(queries, keys, values, lengths)
    outs = []
    for group in groups:
        final = group[-1] == len(bounds) - 1
        outs = receive(
            [arrived[n] for n in group],
            which,
            outs,
            attended if final else None,
            (rows, width),
            blocks,
            [bounds[n] for n in group],
        )
    served, checks, energy, attended = outs
    return served, jnp.transpose(checks, (1, 2, 0)), energy, attended


def local(mantissa, exponent, home, queries, keys, values, lengths):
    rows, width = mantissa.shape[1:]
    mant = mantissa.reshape(rows, width)
    expo = jnp.transpose(exponent, (2, 0, 1))
    branches = [functools.partial(refresh, r) for r in range(1, LARGEST_DISTANCE + 1)]
    served, checks, energy, attended = lax.switch(
        home[0] - 1, branches, mant, expo, queries, keys, values, lengths
    )
    return served[None], checks, energy, attended


def solution(mesh):
    placed = (
        P("blk", "tp", None),
        P("blk", "tp", None),
        P(),
        P("blk", "tp"),
        P("blk", None, "tp"),
        P("blk", None, "tp"),
        P("blk"),
    )
    return jax.shard_map(
        local,
        mesh=mesh,
        in_specs=placed,
        out_specs=(P("blk", "tp", None), P("blk", "tp", None), P("blk"), P("blk", "tp")),
        check_vma=False,
    )
```
